32 devices in a mesh: blk: 8 (over z, core), bond: 4 (over y, x).
Axes of the slice: x: 2, y: 2, z: 4, core: 2. Of those that a mesh axis runs over, the one named last changes fastest.
Arguments:
- iso: bfloat16 [8, 256, 256, 256], P('blk', None, 'bond'), may hold values from -0.03125 to 0.03125
- edge_left: bfloat16 [8, 256, 256], P('blk'), may hold values from -0.375 to 0.375
- edge_right: bfloat16 [8, 256, 256], P('blk'), may hold values from -0.375 to 0.375
- coupling: float32 [8, 256, 256], P('blk'), may hold values from -0.25 to 0.25
Outputs:
- iso_out: bfloat16 [8, 256, 256, 256], P('blk', None, 'bond')
- top_env: float32 [8, 256, 256], P('blk')
The draws below stay inside these ranges and needn't reach their ends.
All inputs are finite; a program needn't handle non-finite values.
Results may differ from the reference program's by a relative error of at most 0.00105.
The reference program's roundings to bfloat16 on the way count: a program that leaves them out, or rounds other values in their place, can miss the bound.
Values may be sent and summed in bfloat16 or wider, within the bound.
A program may use at most 128 MiB of HBM per device.

```python
import math
import jax
import jax.numpy as jnp
from jax import lax

CHI = 256
NEWTON = 2
SUBTREES = 8
LEVELS = 3
CB = 64


def draw_iso(key, part):
    ranks = 4
    sigma = 1.0 / CHI
    block_ids = jnp.arange(CHI, dtype=jnp.int32) // CB
    block_weights = jax.random.uniform(jax.random.fold_in(key, 7001), (ranks, CHI // CB), jnp.float32, 0.0, 1.0)
    per_column = jnp.take(block_weights, block_ids, axis=1)
    strength = 0.5

    def one_subtree(index):
        subkey = jax.random.fold_in(jax.random.fold_in(key, 7002), index)
        first_key, second_key, third_key = jax.random.split(subkey, 3)
        base = jnp.clip(jax.random.normal(first_key, (CHI, CHI, CHI), jnp.float32), -6.0, 6.0)
        shared = jax.random.normal(second_key, (ranks, CHI, CHI), jnp.float32) * per_column[:, None, :]
        columns = jax.random.normal(third_key, (ranks, CHI), jnp.float32)
        common = jnp.einsum('rab,rp->abp', shared, columns) * (strength / math.sqrt(ranks))
        values = jnp.clip(sigma * (base + common), -8.0 * sigma, 8.0 * sigma)
        return values.astype(jnp.bfloat16)
    return lax.map(one_subtree, jnp.arange(SUBTREES, dtype=jnp.int32))


def block_scale(own_key, extent, cuts, smallest, top_value):
    loudness, own = 1.0, jax.random.fold_in(own_key, 6)
    for position, shards_of in cuts:
        draws = jnp.exp(jax.random.uniform(jax.random.fold_in(own, position), (shards_of,), jnp.float32, smallest / len(cuts), top_value / len(cuts)))
        loudness = loudness * jnp.repeat(draws, extent[position] // shards_of).reshape([-1 if axis == position else 1 for axis in range(len(extent))])
    return loudness


def normal_values(own_key, shape, width, reach, pieces=(), held_as=jnp.bfloat16):
    entries = width * jax.random.normal(own_key, shape, jnp.float32)
    if pieces:
        entries = entries * block_scale(own_key, shape, pieces, -0.22, 0.18)
    return jnp.clip(entries, -reach, reach).astype(held_as)


def setup_inputs(seed: int = 0) -> dict:
    key_of = jax.random.split(jax.random.key(seed), 5)
    iso = draw_iso(jax.random.fold_in(key_of[4], 71), 0)
    edge_left = normal_values(key_of[1], (SUBTREES, CHI, CHI), CHI ** -0.5, 0.375, ((0, 8),))
    edge_right = normal_values(key_of[2], (SUBTREES, CHI, CHI), CHI ** -0.5, 0.375, ((0, 8),))
    coupling = normal_values(key_of[3], (SUBTREES, CHI, CHI), (2 * CHI) ** -0.5, 0.25, ((0, 8),), jnp.float32)
    return {"iso": iso, "edge_left": edge_left, "edge_right": edge_right, "coupling": coupling}


highest = lax.Precision.HIGHEST

def ascend_pair(packed):
    iso_one, left_one, right_one = packed
    wide_iso = iso_one.astype(jnp.float32)
    operators = jnp.stack([left_one, right_one]).astype(jnp.float32)
    mapped = jnp.einsum('kxa,abp->kxbp', operators, wide_iso, precision=highest)
    return jnp.einsum('abp,kabq->kpq', wide_iso, mapped, precision=highest)

def update_one(packed):
    iso_one, mix_one, top_one = packed
    wide_iso = iso_one.astype(jnp.float32)
    gradient = jnp.einsum('xa,abp->xbp', mix_one.astype(jnp.float32), wide_iso, precision=highest)
    gradient = gradient + jnp.einsum('abq,qp->abp', wide_iso, top_one.astype(jnp.float32), precision=highest)
    flattened = gradient.reshape(CHI * CHI, CHI)
    flattened = flattened * lax.rsqrt(jnp.sum(flattened * flattened) + 1e-06)
    for newton_step in range(NEWTON):
        gram_mat = jnp.dot(flattened.T, flattened, precision=highest)
        flattened = 1.5 * flattened - 0.5 * jnp.dot(flattened, gram_mat, precision=highest)
    return flattened.reshape(CHI, CHI, CHI).astype(jnp.bfloat16)

def reference(iso, edge_left, edge_right, coupling):
    ascended = lax.map(ascend_pair, (iso, edge_left, edge_right)).astype(jnp.bfloat16)
    left_bounds = ascended[:, 0]
    right_bounds = ascended[:, 1]
    environ = left_bounds.astype(jnp.float32) + right_bounds.astype(jnp.float32)
    subtree_ids = jnp.arange(SUBTREES, dtype=jnp.int32)
    for level_idx in range(LEVELS):
        partner = environ[jnp.bitwise_xor(subtree_ids, 1 << level_idx)]
        mapped = jnp.einsum('sij,sjk,slk->sil', coupling, partner, coupling, precision=highest)
        environ = 0.5 * (environ + mapped)
    top_low = environ.astype(jnp.bfloat16)
    mixed_op = edge_left.astype(jnp.float32) + jnp.roll(right_bounds, 1, axis=0).astype(jnp.float32)
    mixed_op = (mixed_op + jnp.roll(left_bounds, -1, axis=0).astype(jnp.float32)).astype(jnp.bfloat16)
    iso_out = lax.map(update_one, (iso, mixed_op, top_low))
    return (iso_out, environ)
```

```python
import jax
import jax.numpy as jnp
from jax import lax
from jax.experimental import pallas as pl
from jax.experimental.pallas import tpu as pltpu
from jax.sharding import PartitionSpec as P

NEWTON = 2
CHUNK = 16

highest = lax.Precision.HIGHEST
f32 = jnp.float32
bf16 = jnp.bfloat16


def shifted(block, axis, distance):
    devices = range(lax.axis_size(axis))
    route = [((i - distance) % len(devices), i) for i in devices]
    return lax.ppermute(block, axis, route)


def partner_2(block, axis, stride):
    count = lax.axis_size(axis)
    route = []
    for low in range(count):
        high = low | 1 << stride
        if high != low and high < count:
            route += [(low, high), (high, low)]
    return lax.ppermute(block, axis, route)


def mm(a, b):
    return jnp.dot(a, b, preferred_element_type=f32)


def tmm(a, b):
    return lax.dot_general(a, b, (((0,), (0,)), ((), ())), preferred_element_type=f32)


def ascend_kernel(iso_ref, edges_ref, rows_ref, total_ref):
    @pl.when(pl.program_id(0) == 0)
    def _():
        total_ref[...] = jnp.zeros_like(total_ref)

    chi = iso_ref.shape[0]
    rows_ref[...] = jnp.transpose(iso_ref[...], (1, 0, 2))

    def step(b, carry):
        one = rows_ref[b]
        for k in range(2):
            mapped = mm(edges_ref[k], one)
            high = mapped.astype(bf16)
            low = (mapped - high.astype(f32)).astype(bf16)
            total_ref[k] += tmm(one, high) + tmm(one, low)
        return carry

    lax.fori_loop(0, rows_ref.shape[0], step, 0, unroll=4)


def gram_kernel(rows_ref, mix_ref, top_ref, gram_ref):
    @pl.when(pl.program_id(0) == 0)
    def _():
        gram_ref[...] = jnp.zeros_like(gram_ref)

    def step(b, carry):
        one = rows_ref[b]
        grad = (mm(mix_ref[...], one) + mm(one, top_ref[...])).astype(bf16)
        gram_ref[...] += tmm(grad, grad)
        return carry

    lax.fori_loop(0, rows_ref.shape[0], step, 0, unroll=4)


def update_kernel(rows_ref, mix_ref, top_ref, rest_ref, mean_ref, out_ref, held_ref):
    mean = mean_ref[0, 0]

    def step(b, carry):
        one = rows_ref[b]
        grad = mm(mix_ref[...], one) + mm(one, top_ref[...])
        held_ref[b] = (mean * grad + mm(grad.astype(bf16), rest_ref[...])).astype(bf16)
        return carry

    lax.fori_loop(0, rows_ref.shape[0], step, 0, unroll=4)
    out_ref[...] = jnp.transpose(held_ref[...], (1, 0, 2))


def whole(shape):
    return pl.BlockSpec(shape, lambda i: (0,) * len(shape))


def body(iso, edge_left, edge_right, coupling):
    iso = iso[0]
    chi, depth, _ = iso.shape
    chunk = CHUNK if depth % CHUNK == 0 else depth
    steps = depth // chunk
    square = (chi, chi)
    iso_spec = pl.BlockSpec((chi, chunk, chi), lambda i: (0, i, 0))
    rows_spec = pl.BlockSpec((chunk, chi, chi), lambda i: (i, 0, 0))
    params = pltpu.CompilerParams(
        dimension_semantics=("arbitrary",), vmem_limit_bytes=48 * 1024 * 1024
    )
    work = 2 * depth * chi**3
    edges = jnp.stack([edge_left[0], edge_right[0]])
    rows, partial_value = pl.pallas_call(
        ascend_kernel,
        grid=(steps,),
        in_specs=[iso_spec, whole((2, *square))],
        out_specs=[rows_spec, whole((2, *square))],
        out_shape=[
            jax.ShapeDtypeStruct((depth, *square), bf16),
            jax.ShapeDtypeStruct((2, *square), f32),
        ],
        compiler_params=params,
        cost_estimate=pl.CostEstimate(flops=6 * work, bytes_accessed=4 * iso.size, transcendentals=0),
        name="ascend",
    )(iso, edges)
    ranks = lax.axis_size("bond")
    pieces = partial_value.reshape(ranks, -1, chi)
    pieces = lax.all_to_all(pieces, "bond", 0, 0, tiled=True)
    piece = jnp.sum(pieces, axis=0).astype(bf16)
    bounds = lax.all_gather(piece, "bond", axis=0, tiled=True).reshape(2, *square)
    own_left = bounds[0]
    own_right = bounds[1]
    from_left = shifted(own_right, "blk", 1)
    from_right = shifted(own_left, "blk", -1)
    environ = own_left.astype(f32) + own_right.astype(f32)
    couple_mat = coupling[0]
    for level_idx in range(lax.axis_size("blk").bit_length() - 1):
        partner = partner_2(environ, "blk", level_idx)
        carried = jnp.dot(
            jnp.dot(couple_mat, partner, precision=highest), couple_mat.T, precision=highest
        )
        environ = 0.5 * (environ + carried)
    top_low = environ.astype(bf16)
    mixed_op = edge_left[0].astype(f32) + from_left.astype(f32) + from_right.astype(f32)
    mixed_op = mixed_op.astype(bf16)
    part_gram = pl.pallas_call(
        gram_kernel,
        grid=(steps,),
        in_specs=[rows_spec, whole(square), whole(square)],
        out_specs=whole(square),
        out_shape=jax.ShapeDtypeStruct(square, f32),
        compiler_params=params,
        cost_estimate=pl.CostEstimate(flops=3 * work, bytes_accessed=2 * iso.size, transcendentals=0),
        name="gram",
    )(rows, mixed_op, top_low)
    left = jnp.trace(part_gram)
    extra = []
    for _ in range(3):
        head = lax.reduce_precision(left, 8, 7)
        extra.append(jnp.full((1, chi), head, f32))
        left = left - head
    packed = jnp.concatenate([part_gram, *extra, jnp.zeros((13, chi), f32)], axis=0).astype(bf16)
    packed = lax.all_gather(packed, "bond", axis=0).astype(f32)
    packed = jnp.sum(packed, axis=0)
    squares = packed[chi, 0] + packed[chi + 1, 0] + packed[chi + 2, 0]
    scale = lax.rsqrt(squares + 1e-06)
    first_gram = packed[:chi] * (scale * scale)
    gram = first_gram
    eye = jnp.eye(chi, dtype=f32)
    total = eye
    for newton_step in range(NEWTON):
        step = 1.5 * eye - 0.5 * gram
        total = step if newton_step == 0 else jnp.dot(total, step, precision=highest)
        if newton_step + 1 < NEWTON:
            gram = jnp.dot(jnp.dot(step, gram, precision=highest), step, precision=highest)
    mean = jnp.sum(first_gram * total) / jnp.maximum(jnp.trace(first_gram), 1e-30)
    rest = ((total - mean * eye) * scale).astype(bf16)
    updated = pl.pallas_call(
        update_kernel,
        grid=(steps,),
        in_specs=[
            rows_spec,
            whole(square),
            whole(square),
            whole(square),
            pl.BlockSpec(memory_space=pltpu.SMEM),
        ],
        out_specs=iso_spec,
        out_shape=jax.ShapeDtypeStruct(iso.shape, bf16),
        scratch_shapes=[pltpu.VMEM((chunk, *square), bf16)],
        compiler_params=params,
        cost_estimate=pl.CostEstimate(flops=3 * work, bytes_accessed=4 * iso.size, transcendentals=0),
        name="update",
    )(rows, mixed_op, top_low, rest, (mean * scale).reshape(1, 1))
    return (updated[None], environ[None])


def solution(mesh):
    placed = (
        P("blk", None, "bond", None),
        P("blk", None, None),
        P("blk", None, None),
        P("blk", None, None),
    )
    return jax.shard_map(
        body,
        mesh=mesh,
        in_specs=placed,
        out_specs=(P("blk", None, "bond", None), P("blk", None, None)),
        check_vma=False,
    )
```

```python
import jax
import jax.numpy as jnp
from jax import lax
from jax.experimental import pallas as pl
from jax.experimental.pallas import tpu as pltpu
from jax.sharding import PartitionSpec as P

NEWTON = 2
CHUNK = 16
GROUP = 4
TAIL = 16

highest = lax.Precision.HIGHEST
f32 = jnp.float32
bf16 = jnp.bfloat16


def shifted(block, axis, distance):
    devices = range(lax.axis_size(axis))
    route = [((i - distance) % len(devices), i) for i in devices]
    return lax.ppermute(block, axis, route)


def partner_2(block, axis, stride):
    count = lax.axis_size(axis)
    route = []
    for low in range(count):
        high = low | 1 << stride
        if high != low and high < count:
            route += [(low, high), (high, low)]
    return lax.ppermute(block, axis, route)


def mm(a, b):
    return jnp.dot(a, b, preferred_element_type=f32)


def ascend_kernel(iso_ref, edges_ref, rows_ref, total_ref):
    @pl.when(pl.program_id(0) == 0)
    def _():
        total_ref[...] = jnp.zeros_like(total_ref)

    chi = iso_ref.shape[0]
    rows_ref[...] = jnp.transpose(iso_ref[...], (1, 0, 2))

    def step(g, carry):
        mats = [rows_ref[g * GROUP + j] for j in range(GROUP)]
        turned = jnp.concatenate(mats, axis=0).T
        mapped = [mm(edges_ref[...], one) for one in mats]
        for k in range(2):
            both = jnp.concatenate([part[k * chi : (k + 1) * chi] for part in mapped], axis=0)
            high = both.astype(bf16)
            low = (both - high.astype(f32)).astype(bf16)
            total_ref[k] += mm(turned, high) + mm(turned, low)
        return carry

    lax.fori_loop(0, rows_ref.shape[0] // GROUP, step, 0, unroll=2)


def gram_kernel(rows_ref, mix_ref, self_ref, cross_ref, plain_ref):
    @pl.when(pl.program_id(0) == 0)
    def _():
        for ref in (self_ref, cross_ref, plain_ref):
            ref[...] = jnp.zeros_like(ref)

    def step(g, carry):
        mats = [rows_ref[g * GROUP + j] for j in range(GROUP)]
        rows = jnp.concatenate(mats, axis=0)
        moved = jnp.concatenate([mm(mix_ref[...], one).astype(bf16) for one in mats], axis=0)
        turned = moved.T
        self_ref[...] += mm(turned, moved)
        cross_ref[...] += mm(turned, rows)
        plain_ref[...] += mm(rows.T, rows)
        return carry

    lax.fori_loop(0, rows_ref.shape[0] // GROUP, step, 0, unroll=2)


def exact(a, b):
    return jnp.dot(a, b, precision=highest, preferred_element_type=f32)


def diagonal(shape):
    return lax.broadcasted_iota(jnp.int32, shape, 0) == lax.broadcasted_iota(jnp.int32, shape, 1)


def join_kernel(self_ref, cross_ref, plain_ref, top_ref, packed_ref):
    chi = self_ref.shape[0]
    top = top_ref[...].astype(f32)
    half = exact(cross_ref[...] + 0.5 * exact(top.T, plain_ref[...]), top)
    gram = self_ref[...] + half + half.T
    packed_ref[0:chi, :] = gram.astype(bf16)
    trace = jnp.sum(jnp.where(diagonal(gram.shape), gram, 0.0), keepdims=True)
    left = jnp.broadcast_to(trace, (TAIL, chi))
    place = lax.broadcasted_iota(jnp.int32, (TAIL, chi), 0)
    tail = jnp.zeros((TAIL, chi), f32)
    for row in range(3):
        head = left.astype(bf16).astype(f32)
        tail = jnp.where(place == row, head, tail)
        left = left - head
    packed_ref[chi : chi + TAIL, :] = tail.astype(bf16)


def update_kernel(rows_ref, mix_ref, top_ref, packed_ref, out_ref, held_ref, rest_ref, mean_ref):
    @pl.when(pl.program_id(0) == 0)
    def _():
        chi = mix_ref.shape[0]
        packed = packed_ref[0].astype(f32)
        for rank in range(1, packed_ref.shape[0]):
            packed = packed + packed_ref[rank].astype(f32)
        squares = jnp.sum(packed[chi:], axis=0, keepdims=True)
        scale = lax.rsqrt(squares + 1e-06)
        first_gram = packed[:chi] * (scale * scale)
        gram = first_gram
        eye = diagonal(gram.shape).astype(f32)
        total = eye
        for newton_step in range(NEWTON):
            step = 1.5 * eye - 0.5 * gram
            total = step if newton_step == 0 else exact(total, step)
            if newton_step + 1 < NEWTON:
                gram = exact(exact(step, gram), step)
        energy = jnp.sum(first_gram * eye, keepdims=True)
        mean = jnp.sum(first_gram * total, keepdims=True) / jnp.maximum(energy, 1e-30)
        rest_ref[...] = ((total - mean * eye) * scale).astype(bf16)
        mean_ref[...] = mean * scale

    mean = mean_ref[...]

    def step(g, carry):
        mats = [rows_ref[g * GROUP + j] for j in range(GROUP)]
        rows = jnp.concatenate(mats, axis=0)
        moved = jnp.concatenate([mm(mix_ref[...], one) for one in mats], axis=0)
        grad = moved + mm(rows, top_ref[...])
        done = (mean * grad + mm(grad.astype(bf16), rest_ref[...])).astype(bf16)
        held_ref[pl.ds(g * GROUP, GROUP)] = done.reshape(GROUP, *mix_ref.shape)
        return carry

    lax.fori_loop(0, rows_ref.shape[0] // GROUP, step, 0, unroll=2)
    out_ref[...] = jnp.transpose(held_ref[...], (1, 0, 2))


def whole(shape):
    return pl.BlockSpec(shape, lambda i: (0,) * len(shape))


def body(iso, edge_left, edge_right, coupling):
    iso = iso[0]
    chi, depth, _ = iso.shape
    chunk = CHUNK if depth % CHUNK == 0 else depth
    steps = depth // chunk
    square = (chi, chi)
    iso_spec = pl.BlockSpec((chi, chunk, chi), lambda i: (0, i, 0))
    rows_spec = pl.BlockSpec((chunk, chi, chi), lambda i: (i, 0, 0))
    params = pltpu.CompilerParams(
        dimension_semantics=("arbitrary",), vmem_limit_bytes=48 * 1024 * 1024
    )
    work = 2 * depth * chi**3
    edges = jnp.concatenate([edge_left[0], edge_right[0]], axis=0)
    rows, partial_value = pl.pallas_call(
        ascend_kernel,
        grid=(steps,),
        in_specs=[iso_spec, whole((2 * chi, chi))],
        out_specs=[rows_spec, whole((2, *square))],
        out_shape=[
            jax.ShapeDtypeStruct((depth, *square), bf16),
            jax.ShapeDtypeStruct((2, *square), f32),
        ],
        compiler_params=params,
        cost_estimate=pl.CostEstimate(flops=6 * work, bytes_accessed=4 * iso.size, transcendentals=0),
        name="ascend",
    )(iso, edges)
    ranks = lax.axis_size("bond")
    pieces = partial_value.reshape(ranks, -1, chi)
    pieces = lax.all_to_all(pieces, "bond", 0, 0, tiled=True)
    piece = jnp.sum(pieces, axis=0).astype(bf16)
    bounds = lax.all_gather(piece, "bond", axis=0, tiled=True).reshape(2, *square)
    own_left = bounds[0]
    own_right = bounds[1]
    from_left = shifted(own_right, "blk", 1)
    from_right = shifted(own_left, "blk", -1)
    mixed_op = edge_left[0].astype(f32) + from_left.astype(f32) + from_right.astype(f32)
    mixed_op = mixed_op.astype(bf16)
    environ = own_left.astype(f32) + own_right.astype(f32)
    couple_mat = coupling[0]
    levels = lax.axis_size("blk").bit_length() - 1
    for level_idx in range(levels):
        if level_idx == levels - 1:
            environ, mixed_op = lax.optimization_barrier((environ, mixed_op))
        partner = partner_2(environ, "blk", level_idx)
        carried = jnp.dot(
            jnp.dot(couple_mat, partner, precision=highest), couple_mat.T, precision=highest
        )
        environ = 0.5 * (environ + carried)
    grams = pl.pallas_call(
        gram_kernel,
        grid=(steps,),
        in_specs=[rows_spec, whole(square)],
        out_specs=[whole(square)] * 3,
        out_shape=[jax.ShapeDtypeStruct(square, f32)] * 3,
        compiler_params=params,
        cost_estimate=pl.CostEstimate(flops=4 * work, bytes_accessed=2 * iso.size, transcendentals=0),
        name="gram",
    )(rows, mixed_op)
    top_low = environ.astype(bf16)
    packed = pl.pallas_call(
        join_kernel,
        out_shape=jax.ShapeDtypeStruct((chi + TAIL, chi), bf16),
        compiler_params=pltpu.CompilerParams(vmem_limit_bytes=8 * 1024 * 1024),
        name="join",
    )(*grams, top_low)
    packed = lax.all_gather(packed, "bond", axis=0)
    updated = pl.pallas_call(
        update_kernel,
        grid=(steps,),
        in_specs=[rows_spec, whole(square), whole(square), whole(packed.shape)],
        out_specs=iso_spec,
        out_shape=jax.ShapeDtypeStruct(iso.shape, bf16),
        scratch_shapes=[
            pltpu.VMEM((chunk, *square), bf16),
            pltpu.VMEM(square, bf16),
            pltpu.VMEM((1, chi), f32),
        ],
        compiler_params=params,
        cost_estimate=pl.CostEstimate(flops=3 * work, bytes_accessed=4 * iso.size, transcendentals=0),
        name="update",
    )(rows, mixed_op, top_low, packed)
    return (updated[None], environ[None])


def solution(mesh):
    placed = (
        P("blk", None, "bond", None),
        P("blk", None, None),
        P("blk", None, None),
        P("blk", None, None),
    )
    return jax.shard_map(
        body,
        mesh=mesh,
        in_specs=placed,
        out_specs=(P("blk", None, "bond", None), P("blk", None, None)),
        check_vma=False,
    )
```
